8 devices in a mesh: pod: 1 (over z), data: 2 (over y), tensor: 4 (over x, core).
Axes of the slice: x: 2, y: 2, z: 1, core: 2. Of those that a mesh axis runs over, the one named last changes fastest.
Arguments:
- token_ids: int32 [8192], P(('pod', 'data'))
- embed_table: bfloat16 [151936, 896], P('tensor')
- norm_gain: bfloat16 [896], replicated
- w_in: bfloat16 [896, 4864], P(None, 'tensor')
- w_out: bfloat16 [4864, 896], P('tensor')
- d_out: bfloat16 [8192, 896], P(('pod', 'data', 'tensor'))
Outputs:
- output 1: bfloat16 [8192, 896], P(('pod', 'data', 'tensor'))
- output 2: float32 [151936, 896], P(('pod', 'tensor'))
- output 3: float32 [896, 4864], P('pod', 'tensor')
- output 4: float32 [4864, 896], P(('pod', 'tensor'))
All inputs are finite; a program needn't handle non-finite values.
Results may differ from the reference program's by a relative error of at most 0.00578052.
Values are sent between devices in bfloat16 or wider.
A program may use at most 1 GiB of HBM per device.

```python
import jax
import jax.numpy as jnp
from jax import lax

DATA_WAYS = 2
TENSOR_WAYS = 4
TOK_DEV = 1024
VOCAB_SIZE = 151936
MODEL_DIM = 896
FFN_DIM = 4864
NORM_EPS = 1e-6
TOKENS_REP = TOK_DEV * TENSOR_WAYS


def gelu_tanh(value):
    return jax.nn.gelu(value, approximate=True)


def draw_ids(id_key):
    k_base, k_shift, k_hot, k_pick, k_use = jax.random.split(id_key, 5)
    total_tok = DATA_WAYS * TOKENS_REP
    base_ids = jax.random.randint(k_base, (total_tok,), 0, VOCAB_SIZE)
    shift_by = jax.random.randint(k_shift, (total_tok,), 0, 3)
    skewed = jnp.right_shift(base_ids, shift_by)
    hot_ids = jax.random.randint(k_hot, (16,), 0, VOCAB_SIZE)
    hot_pick = jax.random.randint(k_pick, (total_tok,), 0, 16)
    use_hot = jax.random.randint(k_use, (total_tok,), 0, 4) == 0
    token_ids = jnp.where(use_hot, hot_ids[hot_pick], skewed)
    token_ids = token_ids.at[0].set(0).at[total_tok - 1].set(VOCAB_SIZE - 1)
    return token_ids.astype(jnp.int32)


def setup_inputs(seed: int = 0, part: int = 0) -> dict:
    root_key = jax.random.key(seed)
    k_table, k_gain, k_in, k_out, k_part = jax.random.split(root_key, 5)
    k_ids, k_grad = jax.random.split(jax.random.fold_in(k_part, part))
    total_tok = DATA_WAYS * TOKENS_REP
    embed_table = jax.random.normal(k_table, (VOCAB_SIZE, MODEL_DIM), jnp.float32).astype(jnp.bfloat16)
    norm_gain = (1.0 + 0.5 * jax.random.uniform(k_gain, (MODEL_DIM,), jnp.float32, -1.0, 1.0)).astype(jnp.bfloat16)
    w_in = (jax.random.normal(k_in, (MODEL_DIM, FFN_DIM), jnp.float32) * MODEL_DIM ** -0.5).astype(jnp.bfloat16)
    w_out = (jax.random.normal(k_out, (FFN_DIM, MODEL_DIM), jnp.float32) * (1.5 * FFN_DIM ** -0.5)).astype(jnp.bfloat16)
    d_out = jax.random.normal(k_grad, (total_tok, MODEL_DIM), jnp.float32).astype(jnp.bfloat16)
    return {"token_ids": draw_ids(k_ids), "embed_table": embed_table, "norm_gain": norm_gain, "w_in": w_in, "w_out": w_out, "d_out": d_out}


def reference(token_ids, embed_table, norm_gain, w_in, w_out, d_out):
    blocks = DATA_WAYS * TENSOR_WAYS
    embedded = jnp.take(embed_table, token_ids, axis=0).reshape(blocks, TOK_DEV, MODEL_DIM)
    grad_blocks = d_out.reshape(blocks, TOK_DEV, MODEL_DIM)
    gain_f32 = norm_gain.astype(jnp.float32)

    def block_step(acc_pair, step_in):
        acc_w_in, acc_w_out = acc_pair
        x_blk, dy_blk = step_in
        x_f32 = x_blk.astype(jnp.float32)
        inv_rms = lax.rsqrt(jnp.mean(x_f32 * x_f32, axis=-1, keepdims=True) + NORM_EPS)
        x_hat = x_f32 * inv_rms
        normed = (x_hat * gain_f32).astype(jnp.bfloat16)
        pre_gelu = jnp.dot(normed, w_in, preferred_element_type=jnp.float32).astype(jnp.bfloat16)
        hidden_f32, gelu_pull = jax.vjp(gelu_tanh, pre_gelu.astype(jnp.float32))
        hidden = hidden_f32.astype(jnp.bfloat16)
        mlp_out = jnp.dot(hidden, w_out, preferred_element_type=jnp.float32)
        out_blk = (x_f32 + mlp_out).astype(jnp.bfloat16)
        grad_hidden = jnp.dot(dy_blk, w_out.T, preferred_element_type=jnp.float32)
        grad_pre = gelu_pull(grad_hidden)[0].astype(jnp.bfloat16)
        acc_w_out = acc_w_out + jnp.dot(hidden.T, dy_blk, preferred_element_type=jnp.float32)
        acc_w_in = acc_w_in + jnp.dot(normed.T, grad_pre, preferred_element_type=jnp.float32)
        d_normed = jnp.dot(grad_pre, w_in.T, preferred_element_type=jnp.float32)
        d_hat = d_normed * gain_f32
        d_norm_in = inv_rms * (d_hat - x_hat * jnp.mean(d_hat * x_hat, axis=-1, keepdims=True))
        dx_blk = (dy_blk.astype(jnp.float32) + d_norm_in).astype(jnp.bfloat16)
        return (acc_w_in, acc_w_out), (out_blk, dx_blk)

    zeros_in = jnp.zeros((MODEL_DIM, FFN_DIM), jnp.float32)
    zeros_out = jnp.zeros((FFN_DIM, MODEL_DIM), jnp.float32)
    (grad_w_in, grad_w_out), (out_blocks, dx_blocks) = lax.scan(block_step, (zeros_in, zeros_out), (embedded, grad_blocks))
    grad_table = jax.ops.segment_sum(dx_blocks.reshape(-1, MODEL_DIM).astype(jnp.float32), token_ids, num_segments=VOCAB_SIZE)
    return out_blocks.reshape(-1, MODEL_DIM), grad_table, grad_w_in, grad_w_out
```

```python
import functools

import jax
import jax.numpy as jnp
from jax import lax
from jax.experimental import pallas as pl
from jax.experimental.pallas import tpu as pltpu
from jax.sharding import PartitionSpec as P


NORM_EPS = 1e-6
LOOK_BLOCK = 256
LOOK_GROUP = 32
LOOK_DEPTH = 3
ISSUE = 16
TABLE_BLOCK = 2048
WIDEN_ROWS = 256
LOAD_DEPTH = 3
UNROLL = 8


def gelu_tanh(value):
    return jax.nn.gelu(value, approximate=True)


def lookup_kernel(base, row_ref, count_ref, code_ref, table_ref, out_ref, tiles, sems):
    step, steps = pl.program_id(0), pl.num_programs(0)

    def fetch(block):
        slot = lax.rem(block, LOOK_DEPTH)
        first = (base + block) * LOOK_BLOCK

        def some(j, carry):
            for k in range(ISSUE):
                row = row_ref[first + j * ISSUE + k]

                @pl.when(row >= 0)
                def _():
                    pltpu.make_async_copy(
                        table_ref.at[pl.ds(pl.multiple_of(row, 8), 8), :],
                        tiles.at[slot * LOOK_BLOCK + j * ISSUE + k],
                        sems.at[slot],
                    ).start()

            return carry

        lax.fori_loop(0, LOOK_BLOCK // ISSUE, some, 0)

    @pl.when(step == 0)
    def _():
        def clear(i, carry):
            tiles[pl.ds(i * LOOK_GROUP, LOOK_GROUP)] = jnp.zeros((LOOK_GROUP,) + tiles.shape[1:], tiles.dtype)
            return carry

        lax.fori_loop(0, LOOK_DEPTH * LOOK_BLOCK // LOOK_GROUP, clear, 0)

        def first(slot, carry):
            fetch(slot)
            return carry

        lax.fori_loop(0, jnp.minimum(LOOK_DEPTH - 1, steps), first, 0)

    @pl.when(step + LOOK_DEPTH - 1 < steps)
    def _():
        fetch(step + LOOK_DEPTH - 1)

    slot = lax.rem(step, LOOK_DEPTH)
    count = count_ref[base + step]

    @pl.when(count > 0)
    def _():
        fetched = tiles.at[pl.ds(0, count)]
        pltpu.make_async_copy(fetched, fetched, sems.at[slot]).wait()

    places = lax.broadcasted_iota(jnp.int32, (LOOK_GROUP * 8, LOOK_GROUP), 0)

    for j in range(LOOK_BLOCK // LOOK_GROUP):
        group = pl.ds(j * LOOK_GROUP, LOOK_GROUP)
        pick = (places == code_ref[pl.ds(j, 1), :]).astype(jnp.bfloat16)
        rows = tiles[pl.ds(slot * LOOK_BLOCK + j * LOOK_GROUP, LOOK_GROUP)].reshape(LOOK_GROUP * 8, -1)
        out_ref[group, :] = dot(pick, rows, COLS_BY_COLS).astype(out_ref.dtype)


def lookup_plan(ids, rank, shard_rows):
    local = ids - rank * shard_rows
    owned = (local >= 0) & (local < shard_rows)
    place = lax.broadcasted_iota(jnp.int32, (ids.shape[0] // LOOK_GROUP, LOOK_GROUP), 1) * 8
    code = jnp.where(owned, local & 7, -1 << 20).reshape(place.shape) + place
    row = jnp.where(owned, local & ~7, -1)
    counts = jnp.sum(owned.reshape(-1, LOOK_BLOCK), axis=1).astype(jnp.int32)
    return row, counts, code


def lookup(plan, table, base, count):
    dim = table.shape[1]
    base //= LOOK_BLOCK
    return pl.pallas_call(
        functools.partial(lookup_kernel, base),
        out_shape=jax.ShapeDtypeStruct((count, dim), table.dtype),
        grid_spec=pltpu.PrefetchScalarGridSpec(
            num_scalar_prefetch=2,
            grid=(count // LOOK_BLOCK,),
            in_specs=[
                pl.BlockSpec((LOOK_BLOCK // LOOK_GROUP, LOOK_GROUP), lambda i, r, c: (base + i, 0)),
                pl.BlockSpec(memory_space=pl.ANY),
            ],
            out_specs=pl.BlockSpec((LOOK_BLOCK, dim), lambda i, r, c: (i, 0)),
            scratch_shapes=[
                pltpu.VMEM((LOOK_DEPTH * LOOK_BLOCK, 8, dim), table.dtype),
                pltpu.SemaphoreType.DMA((LOOK_DEPTH,)),
            ],
        ),
        cost_estimate=pl.CostEstimate(flops=count * 5_000_000, bytes_accessed=count * dim * 18, transcendentals=0),
        name="lookup",
    )(*plan, table)


def norm_kernel(kept_ref, got_ref, away_ref, gain_ref, x_ref, normed_ref):
    x = kept_ref[...].astype(jnp.float32) + got_ref[...].astype(jnp.float32) + away_ref[...].astype(jnp.float32)
    x_ref[...] = x.astype(x_ref.dtype)
    inv_rms = lax.rsqrt(jnp.mean(x * x, axis=-1, keepdims=True) + NORM_EPS)
    normed_ref[...] = (x * inv_rms * gain_ref[...]).astype(normed_ref.dtype)


def norm(kept, got, away, gain):
    rows, dim = away.shape
    tile = rows // 2
    here = pl.BlockSpec((tile, dim), lambda i: (i, 0))
    home = pl.BlockSpec((tile, dim), lambda i: (2 + i, 0))
    return pl.pallas_call(
        norm_kernel,
        out_shape=[jax.ShapeDtypeStruct((rows, dim), away.dtype)] * 2,
        grid=(2,),
        in_specs=[home, home, here, pl.BlockSpec((1, dim), lambda i: (0, 0))],
        out_specs=[here, here],
        cost_estimate=pl.CostEstimate(flops=2_000_000_000, bytes_accessed=rows * dim * 10, transcendentals=rows),
        name="norm",
    )(kept, got, away, gain)


def dx_kernel(place_ref, part_ref, got_ref, away_ref, x_ref, grad_ref, gain_ref, dx_ref):
    d_normed = (part_ref[...] + got_ref[...]) + away_ref[...]
    x = x_ref[...].astype(jnp.float32)
    inv_rms = lax.rsqrt(jnp.mean(x * x, axis=-1, keepdims=True) + NORM_EPS)
    x_hat = x * inv_rms
    d_hat = d_normed * gain_ref[...]
    d_norm_in = inv_rms * (d_hat - x_hat * jnp.mean(d_hat * x_hat, axis=-1, keepdims=True))
    dx_ref[...] = (grad_ref[...].astype(jnp.float32) + d_norm_in).astype(dx_ref.dtype)


def norm_grad(place, part, got, away, x, grad, chunk, gain):
    rows, dim = away.shape
    tile = rows // 2
    plain = pl.BlockSpec((tile, dim), lambda i, p: (i, 0))
    return pl.pallas_call(
        dx_kernel,
        out_shape=jax.ShapeDtypeStruct((rows, dim), x.dtype),
        grid_spec=pltpu.PrefetchScalarGridSpec(
            num_scalar_prefetch=1,
            grid=(2,),
            in_specs=[
                pl.BlockSpec((None, None, tile, dim), lambda i, p: (p[0], p[1], i, 0)),
                pl.BlockSpec((None, tile, dim), lambda i, p: (p[0], i, 0)),
                plain,
                plain,
                pl.BlockSpec((tile, dim), lambda i, p: (2 * chunk + i, 0)),
                pl.BlockSpec((1, dim), lambda i, p: (0, 0)),
            ],
            out_specs=plain,
        ),
        cost_estimate=pl.CostEstimate(flops=3_000_000_000, bytes_accessed=rows * dim * 18, transcendentals=rows),
        name="norm_grad",
    )(place, part, got, away, x, grad, gain)


def table_kernel(start_ref, key_ref, flip_ref, *refs):
    *dx_refs, table_ref, rows_f32, stage, sums_f32, sems, out_sems = refs
    block, blocks = pl.program_id(0), pl.num_programs(0)
    part, dim = dx_refs[0].shape
    tokens = len(dx_refs) * part

    @pl.when(block == 0)
    def _():
        def load(i):
            return pltpu.make_async_copy(dx_refs[i], stage.at[i % LOAD_DEPTH], sems.at[i % LOAD_DEPTH])

        for i in range(LOAD_DEPTH - 1):
            load(i).start()
        for i in range(len(dx_refs)):
            if i + LOAD_DEPTH - 1 < len(dx_refs):
                load(i + LOAD_DEPTH - 1).start()
            load(i).wait()

            def widen(j, carry, i=i):
                rows = pl.ds(pl.multiple_of(j * WIDEN_ROWS, WIDEN_ROWS), WIDEN_ROWS)
                wide = pl.ds(pl.multiple_of(i * part + j * WIDEN_ROWS, WIDEN_ROWS), WIDEN_ROWS)
                rows_f32[wide, :] = stage[i % LOAD_DEPTH, rows, :].astype(jnp.float32)
                return carry

            lax.fori_loop(0, part // WIDEN_ROWS, widen, 0)

    slot = lax.rem(block, 2)
    whole, rest = table_ref.shape[0] // TABLE_BLOCK, table_ref.shape[0] % TABLE_BLOCK

    def put(i, rows):
        at = lax.rem(i, 2)
        return pltpu.make_async_copy(
            sums_f32.at[at, pl.ds(0, rows), :],
            table_ref.at[pl.ds(pl.multiple_of(i * TABLE_BLOCK, TABLE_BLOCK), rows), :],
            out_sems.at[at],
        )

    @pl.when(block >= 2)
    def _():
        put(block - 2, TABLE_BLOCK).wait()

    def clear(i, carry):
        sums_f32[slot, pl.ds(pl.multiple_of(i * 128, 128), 128), :] = jnp.zeros((128, dim), jnp.float32)
        return carry

    lax.fori_loop(0, TABLE_BLOCK // 128, clear, 0)
    first, last, flip = start_ref[block], start_ref[block + 1], flip_ref[0]

    def add(k, carry):
        previous, total = carry
        key = key_ref[k]
        row = (key // tokens) & (TABLE_BLOCK - 1)
        value = rows_f32[pl.ds((key & (tokens - 1)) ^ flip, 1), :]
        return row, jnp.where(row == previous, total + value, value)

    def group(g, carry):
        sums = []
        for u in range(UNROLL):
            carry = add(first + g * UNROLL + u, carry)
            sums.append(carry)
        for row, total in sums:
            sums_f32[slot, pl.ds(row, 1), :] = total
        return carry

    def single(k, carry):
        carry = add(k, carry)
        sums_f32[slot, pl.ds(carry[0], 1), :] = carry[1]
        return carry

    carry = (jnp.int32(-1), jnp.zeros((1, dim), jnp.float32))
    groups = (last - first) // UNROLL
    carry = lax.fori_loop(0, groups, group, carry)
    lax.fori_loop(first + groups * UNROLL, last, single, carry)

    @pl.when(block < whole)
    def _():
        put(block, TABLE_BLOCK).start()

    @pl.when(block == blocks - 1)
    def _():
        if rest:
            put(block, rest).start()
        if table_ref.shape[0] > TABLE_BLOCK:
            put(block - 1, TABLE_BLOCK).wait()
        put(block, rest or TABLE_BLOCK).wait()


def table_plan(ids, rank, shard_rows):
    tokens = ids.shape[0]
    local = ids - rank * shard_rows
    owned = (local >= 0) & (local < shard_rows)
    blocks = pl.cdiv(shard_rows, TABLE_BLOCK)
    key = jnp.where(owned, local, shard_rows + TABLE_BLOCK) * tokens + jnp.arange(tokens, dtype=jnp.int32)
    key = lax.sort(key)
    bounds = jnp.minimum(jnp.arange(blocks + 1, dtype=jnp.int32) * TABLE_BLOCK, shard_rows) * tokens
    return jnp.sum((key[None, :] < bounds[:, None]).astype(jnp.int32), axis=1), key


def table_grad(start, key, flip, dx_parts, shard_rows):
    part, dim = dx_parts[0].shape
    return pl.pallas_call(
        table_kernel,
        out_shape=jax.ShapeDtypeStruct((shard_rows, dim), jnp.float32),
        grid_spec=pltpu.PrefetchScalarGridSpec(
            num_scalar_prefetch=3,
            grid=(start.shape[0] - 1,),
            in_specs=[pl.BlockSpec(memory_space=pl.ANY)] * len(dx_parts),
            out_specs=pl.BlockSpec(memory_space=pl.ANY),
            scratch_shapes=[
                pltpu.VMEM((len(dx_parts) * part + 8, dim), jnp.float32),
                pltpu.VMEM((LOAD_DEPTH, part, dim), jnp.bfloat16),
                pltpu.VMEM((2, TABLE_BLOCK + 8, dim), jnp.float32),
                pltpu.SemaphoreType.DMA((LOAD_DEPTH,)),
                pltpu.SemaphoreType.DMA((2,)),
            ],
        ),
        compiler_params=pltpu.CompilerParams(vmem_limit_bytes=58 << 20),
        cost_estimate=pl.CostEstimate(flops=60_000_000_000, bytes_accessed=shard_rows * dim * 4, transcendentals=0),
        name="table_grad",
    )(start, key, flip, *dx_parts)


CORE_SWAP = [(0, 1), (1, 0), (2, 3), (3, 2)]
CHIP_SWAP = [(0, 2), (2, 0), (1, 3), (3, 1)]
DATA_SWAP = [(0, 1), (1, 0)]
ROWS_BY_COLS = (((1,), (0,)), ((), ()))
ROWS_BY_ROWS = (((1,), (1,)), ((), ()))
COLS_BY_COLS = (((0,), (0,)), ((), ()))


def dot(a, b, dims):
    return lax.dot_general(a, b, dims, preferred_element_type=jnp.float32)


def after(value, *others):
    return lax.optimization_barrier((value,) + others)[0]


def solution(mesh):
    tok_spec = P(("pod", "data", "tensor"), None)

    def per_device(token_ids, embed_table, norm_gain, w_in, w_out, d_out):
        shard_rows, dim = embed_table.shape
        tok_dev = d_out.shape[0]
        part = tok_dev // 2
        rank, replica = lax.axis_index("tensor"), lax.axis_index("data")
        chip, core = rank // 2, rank % 2
        gain_f32 = norm_gain.astype(jnp.float32)[None]
        place = jnp.stack([chip, core]).astype(jnp.int32)
        places = token_ids.reshape(2, 2, 2, part)
        places = jnp.where(chip == 0, places[::-1], places)
        places = jnp.where(core == 0, places[:, ::-1], places)
        look = lookup_plan(places.transpose(2, 1, 0, 3).reshape(-1), rank, shard_rows)

        def gather(value):
            return lax.all_gather(value, "tensor", axis=0, tiled=True)

        ids_other = lax.ppermute(token_ids, "data", DATA_SWAP)
        ids_low, ids_high = jnp.where(replica == 0, token_ids, ids_other), jnp.where(replica == 0, ids_other, token_ids)
        ids_all = jnp.stack([ids_low, ids_high]).reshape(2, 4, 2, part).transpose(2, 1, 0, 3).reshape(-1)
        start, key = table_plan(ids_all, rank, shard_rows)
        flip = ((rank * 2 + replica) * part).astype(jnp.int32)[None]

        grad_gathered = lax.all_gather(d_out.reshape(2, part, dim), "tensor", axis=1, tiled=True)
        grad_all = [grad_gathered[0], grad_gathered[1]]

        looked, aways = [], []
        for c in range(2):
            sent = lookup(look, embed_table, 4 * c * part, 2 * part)
            got = lax.ppermute(sent, "tensor", CORE_SWAP)
            kept = lookup(look, embed_table, (4 * c + 2) * part, 2 * part)
            looked.append((kept, got))
            aways.append(lax.ppermute(kept[:part] + got[:part], "tensor", CHIP_SWAP))

        embedded, normed_all = [], []
        for c in range(2):
            x, normed = norm(*looked[c], aways[c], gain_f32)
            embedded.append(x)
            normed_all.append(gather(after(normed, grad_gathered)))
        normed_all[0] = after(normed_all[0], key)

        def core_sum(value):
            value = value.reshape(2, 2, part, dim)
            send = lax.dynamic_index_in_dim(value, 1 - core, 1, keepdims=False)
            return value, lax.ppermute(send, "tensor", CORE_SWAP)

        def chip_sum(value, got, wait_for=None):
            mine = lax.dynamic_slice(value, (1 - chip, core, 0, 0), (1, 1, part, dim)).reshape(part, dim)
            away = mine + lax.dynamic_index_in_dim(got, 1 - chip, 0, keepdims=False)
            away = away if wait_for is None else after(away, wait_for)
            return value, got, lax.ppermute(away, "tensor", CHIP_SWAP)

        def up(c):
            return dot(normed_all[c], w_in, ROWS_BY_COLS).astype(jnp.bfloat16)

        def down(c, pre_gelu):
            gelu_pull = jax.vjp(gelu_tanh, pre_gelu.astype(jnp.float32))[1]
            grad_hidden = dot(grad_all[c], w_out, ROWS_BY_ROWS)
            grad_pre = gelu_pull(grad_hidden)[0].astype(jnp.bfloat16)
            norm_part = dot(grad_pre, w_in, ROWS_BY_ROWS)
            return grad_pre, norm_part, core_sum(norm_part)

        def act(pre_gelu):
            return gelu_tanh(pre_gelu.astype(jnp.float32)).astype(jnp.bfloat16)

        pre_0 = up(0)
        grad_pre_0, norm_part_0, d_normed_0 = down(0, pre_0)
        normed_all[1] = after(normed_all[1], norm_part_0)
        pre_1 = up(1)
        hidden = [act(pre_0), act(pre_1)]
        grad_w_out = dot(hidden[0], grad_all[0], COLS_BY_COLS) + dot(hidden[1], grad_all[1], COLS_BY_COLS)
        cut = grad_w_out.shape[0] // 2
        other_out_0 = lax.ppermute(grad_w_out[:cut], "data", DATA_SWAP)
        grad_pre_1, _, d_normed_1 = down(1, after(pre_1, grad_w_out))

        def to_dx(c, sums):
            return norm_grad(place, *sums, embedded[c], d_out, c, gain_f32)

        dx_0 = to_dx(0, chip_sum(*d_normed_0))
        crossed_0 = lax.ppermute(dx_0, "data", DATA_SWAP)
        other_out_1 = lax.ppermute(after(grad_w_out[cut:], dx_0), "data", DATA_SWAP)

        grad_pre = [after(g, dx_0) for g in (grad_pre_0, grad_pre_1)]
        grad_w_in = dot(normed_all[0], grad_pre[0], COLS_BY_COLS) + dot(normed_all[1], grad_pre[1], COLS_BY_COLS)

        y_sums = []
        for c in range(2):
            mlp_part = dot(hidden[c], w_out, ROWS_BY_COLS)
            y_sums.append(core_sum(mlp_part))

        dx_1 = to_dx(1, chip_sum(*d_normed_1))
        crossed_1 = lax.ppermute(dx_1, "data", DATA_SWAP)
        other_in = lax.ppermute(after(grad_w_in, dx_1), "data", DATA_SWAP)

        dx_all = []
        for dx, crossed in ((dx_0, crossed_0), (dx_1, crossed_1)):
            pair = jnp.concatenate([dx, crossed])
            from_core = lax.ppermute(pair, "tensor", CORE_SWAP)
            from_chip = lax.ppermute(pair, "tensor", CHIP_SWAP)
            from_both = lax.ppermute(from_chip, "tensor", CORE_SWAP)
            dx_all += [pair, from_core, from_chip, from_both]
        y_1 = chip_sum(*y_sums[1], wait_for=from_chip)
        y_0 = chip_sum(*y_sums[0], wait_for=from_chip)
        y_sums = [y_0, y_1]
        grad_table = table_grad(start, key, flip, dx_all, shard_rows)

        block_out = []
        for c, (value, got, away) in enumerate(y_sums):
            mine = lax.dynamic_slice(value, (chip, core, 0, 0), (1, 1, part, dim)).reshape(part, dim)
            mlp_out = (mine + lax.dynamic_index_in_dim(got, chip, 0, keepdims=False)) + after(away, grad_table)
            block_out.append((embedded[c].astype(jnp.float32) + mlp_out).astype(jnp.bfloat16))
        block_out = jnp.concatenate(block_out)
        grad_w_in = grad_w_in + after(other_in, grad_table)
        grad_w_out = grad_w_out + jnp.concatenate([other_out_0, after(other_out_1, grad_table)])
        return block_out, grad_table, grad_w_in, grad_w_out

    return jax.shard_map(
        per_device,
        mesh=mesh,
        in_specs=(P(("pod", "data")), P("tensor", None), P(None), P(None, "tensor"), P("tensor", None), tok_spec),
        out_specs=(tok_spec, P(("pod", "tensor"), None), P("pod", "tensor"), P(("pod", "tensor"), None)),
        check_vma=False,
    )
```

```python
import functools

import jax
import jax.numpy as jnp
from jax import lax
from jax.experimental import pallas as pl
from jax.experimental.pallas import tpu as pltpu
from jax.sharding import PartitionSpec as P


NORM_EPS = 1e-6
LOOK_BLOCK = 256
LOOK_GROUP = 32
LOOK_DEPTH = 3
ISSUE = 16
TABLE_BLOCK = 2048
WIDEN_ROWS = 256
LOAD_DEPTH = 3
UNROLL = 8


def gelu_tanh(value):
    return jax.nn.gelu(value, approximate=True)


def lookup_kernel(base, row_ref, count_ref, code_ref, table_ref, out_ref, tiles, sems):
    step, steps = pl.program_id(0), pl.num_programs(0)

    def fetch(block):
        slot = lax.rem(block, LOOK_DEPTH)
        first = (base + block) * LOOK_BLOCK

        def some(j, carry):
            for k in range(ISSUE):
                row = row_ref[first + j * ISSUE + k]

                @pl.when(row >= 0)
                def _():
                    pltpu.make_async_copy(
                        table_ref.at[pl.ds(pl.multiple_of(row, 8), 8), :],
                        tiles.at[slot * LOOK_BLOCK + j * ISSUE + k],
                        sems.at[slot],
                    ).start()

            return carry

        lax.fori_loop(0, LOOK_BLOCK // ISSUE, some, 0)

    @pl.when(step == 0)
    def _():
        def clear(i, carry):
            tiles[pl.ds(i * LOOK_GROUP, LOOK_GROUP)] = jnp.zeros((LOOK_GROUP,) + tiles.shape[1:], tiles.dtype)
            return carry

        lax.fori_loop(0, LOOK_DEPTH * LOOK_BLOCK // LOOK_GROUP, clear, 0)

        def first(slot, carry):
            fetch(slot)
            return carry

        lax.fori_loop(0, jnp.minimum(LOOK_DEPTH - 1, steps), first, 0)

    @pl.when(step + LOOK_DEPTH - 1 < steps)
    def _():
        fetch(step + LOOK_DEPTH - 1)

    slot = lax.rem(step, LOOK_DEPTH)
    count = count_ref[base + step]

    @pl.when(count > 0)
    def _():
        fetched = tiles.at[pl.ds(0, count)]
        pltpu.make_async_copy(fetched, fetched, sems.at[slot]).wait()

    places = lax.broadcasted_iota(jnp.int32, (LOOK_GROUP * 8, LOOK_GROUP), 0)

    for j in range(LOOK_BLOCK // LOOK_GROUP):
        group = pl.ds(j * LOOK_GROUP, LOOK_GROUP)
        pick = (places == code_ref[pl.ds(j, 1), :]).astype(jnp.bfloat16)
        rows = tiles[pl.ds(slot * LOOK_BLOCK + j * LOOK_GROUP, LOOK_GROUP)].reshape(LOOK_GROUP * 8, -1)
        out_ref[group, :] = dot(pick, rows, COLS_BY_COLS).astype(out_ref.dtype)


def lookup_plan(ids, rank, shard_rows):
    local = ids - rank * shard_rows
    owned = (local >= 0) & (local < shard_rows)
    place = lax.broadcasted_iota(jnp.int32, (ids.shape[0] // LOOK_GROUP, LOOK_GROUP), 1) * 8
    code = jnp.where(owned, local & 7, -1 << 20).reshape(place.shape) + place
    row = jnp.where(owned, local & ~7, -1)
    counts = jnp.sum(owned.reshape(-1, LOOK_BLOCK), axis=1).astype(jnp.int32)
    return row, counts, code


def lookup(plan, table, base, count):
    dim = table.shape[1]
    base //= LOOK_BLOCK
    return pl.pallas_call(
        functools.partial(lookup_kernel, base),
        out_shape=jax.ShapeDtypeStruct((count, dim), table.dtype),
        grid_spec=pltpu.PrefetchScalarGridSpec(
            num_scalar_prefetch=2,
            grid=(count // LOOK_BLOCK,),
            in_specs=[
                pl.BlockSpec((LOOK_BLOCK // LOOK_GROUP, LOOK_GROUP), lambda i, r, c: (base + i, 0)),
                pl.BlockSpec(memory_space=pl.ANY),
            ],
            out_specs=pl.BlockSpec((LOOK_BLOCK, dim), lambda i, r, c: (i, 0)),
            scratch_shapes=[
                pltpu.VMEM((LOOK_DEPTH * LOOK_BLOCK, 8, dim), table.dtype),
                pltpu.SemaphoreType.DMA((LOOK_DEPTH,)),
            ],
        ),
        cost_estimate=pl.CostEstimate(flops=count * 5_000_000, bytes_accessed=count * dim * 18, transcendentals=0),
        name="lookup",
    )(*plan, table)


def norm_kernel(kept_ref, got_ref, away_ref, gain_ref, x_ref, normed_ref):
    x = kept_ref[...].astype(jnp.float32) + got_ref[...].astype(jnp.float32) + away_ref[...].astype(jnp.float32)
    x_ref[...] = x.astype(x_ref.dtype)
    inv_rms = lax.rsqrt(jnp.mean(x * x, axis=-1, keepdims=True) + NORM_EPS)
    normed_ref[...] = (x * inv_rms * gain_ref[...]).astype(normed_ref.dtype)


def norm(kept, got, away, gain):
    rows, dim = away.shape
    tile = rows // 2
    here = pl.BlockSpec((tile, dim), lambda i: (i, 0))
    home = pl.BlockSpec((tile, dim), lambda i: (2 + i, 0))
    return pl.pallas_call(
        norm_kernel,
        out_shape=[jax.ShapeDtypeStruct((rows, dim), away.dtype)] * 2,
        grid=(2,),
        in_specs=[home, home, here, pl.BlockSpec((1, dim), lambda i: (0, 0))],
        out_specs=[here, here],
        cost_estimate=pl.CostEstimate(flops=2_000_000_000, bytes_accessed=rows * dim * 10, transcendentals=rows),
        name="norm",
    )(kept, got, away, gain)


def take_piece(piece_refs, held, sems):
    step = pl.program_id(0)

    @pl.when(step == 0)
    def _():
        for i, piece_ref in enumerate(piece_refs):
            pltpu.make_async_copy(piece_ref, held.at[i], sems.at[i]).start()

    pltpu.make_async_copy(piece_refs[0], held.at[step], sems.at[step]).wait()
    return held[step]


def join_kernel(*refs):
    *piece_refs, out_ref, held, sems = refs
    out_ref[...] = take_piece(piece_refs, held, sems)


def join(pieces):
    (rows, dim), count, kind = pieces[0].shape, len(pieces), pieces[0].dtype
    return pl.pallas_call(
        join_kernel,
        out_shape=jax.ShapeDtypeStruct((count * rows, dim), kind),
        grid=(count,),
        in_specs=[pl.BlockSpec(memory_space=pl.ANY)] * count,
        out_specs=pl.BlockSpec((rows, dim), lambda i: (i, 0)),
        scratch_shapes=[pltpu.VMEM((count, rows, dim), kind), pltpu.SemaphoreType.DMA((count,))],
        cost_estimate=pl.CostEstimate(flops=2_000_000_000, bytes_accessed=count * rows * dim * 4, transcendentals=0),
        name="join",
    )(*pieces)


def dx_kernel(part_ref, got_ref, away_ref, x_ref, grad_ref, gain_ref, dx_ref):
    d_normed = (part_ref[...] + got_ref[...]) + away_ref[...]
    x = x_ref[...].astype(jnp.float32)
    inv_rms = lax.rsqrt(jnp.mean(x * x, axis=-1, keepdims=True) + NORM_EPS)
    x_hat = x * inv_rms
    d_hat = d_normed * gain_ref[...]
    d_norm_in = inv_rms * (d_hat - x_hat * jnp.mean(d_hat * x_hat, axis=-1, keepdims=True))
    dx_ref[...] = (grad_ref[...].astype(jnp.float32) + d_norm_in).astype(dx_ref.dtype)


def norm_grad(part, got, away, x, grad, chunk, gain):
    rows, dim = away.shape
    tile = rows // 2
    plain = pl.BlockSpec((tile, dim), lambda i: (i, 0))
    return pl.pallas_call(
        dx_kernel,
        out_shape=jax.ShapeDtypeStruct((rows, dim), x.dtype),
        grid=(2,),
        in_specs=[
            pl.BlockSpec((None, None, tile, dim), lambda i: (0, 0, i, 0)),
            pl.BlockSpec((None, tile, dim), lambda i: (0, i, 0)),
            plain,
            plain,
            pl.BlockSpec((tile, dim), lambda i: (2 * chunk + i, 0)),
            pl.BlockSpec((1, dim), lambda i: (0, 0)),
        ],
        out_specs=plain,
        cost_estimate=pl.CostEstimate(flops=3_000_000_000, bytes_accessed=rows * dim * 18, transcendentals=rows),
        name="norm_grad",
    )(part, got, away, x, grad, gain)


def table_kernel(start_ref, key_ref, flip_ref, *refs):
    *dx_refs, table_ref, rows_f32, stage, sums_f32, sems, out_sems = refs
    block, blocks = pl.program_id(0), pl.num_programs(0)
    part, dim = dx_refs[0].shape
    tokens = len(dx_refs) * part

    @pl.when(block == 0)
    def _():
        def load(i):
            return pltpu.make_async_copy(dx_refs[i], stage.at[i % LOAD_DEPTH], sems.at[i % LOAD_DEPTH])

        for i in range(LOAD_DEPTH - 1):
            load(i).start()
        for i in range(len(dx_refs)):
            if i + LOAD_DEPTH - 1 < len(dx_refs):
                load(i + LOAD_DEPTH - 1).start()
            load(i).wait()

            def widen(j, carry, i=i):
                rows = pl.ds(pl.multiple_of(j * WIDEN_ROWS, WIDEN_ROWS), WIDEN_ROWS)
                wide = pl.ds(pl.multiple_of(i * part + j * WIDEN_ROWS, WIDEN_ROWS), WIDEN_ROWS)
                rows_f32[wide, :] = stage[i % LOAD_DEPTH, rows, :].astype(jnp.float32)
                return carry

            lax.fori_loop(0, part // WIDEN_ROWS, widen, 0)

    slot = lax.rem(block, 2)
    whole, rest = table_ref.shape[0] // TABLE_BLOCK, table_ref.shape[0] % TABLE_BLOCK

    def put(i, rows):
        at = lax.rem(i, 2)
        return pltpu.make_async_copy(
            sums_f32.at[at, pl.ds(0, rows), :],
            table_ref.at[pl.ds(pl.multiple_of(i * TABLE_BLOCK, TABLE_BLOCK), rows), :],
            out_sems.at[at],
        )

    @pl.when(block >= 2)
    def _():
        put(block - 2, TABLE_BLOCK).wait()

    def clear(i, carry):
        sums_f32[slot, pl.ds(pl.multiple_of(i * 128, 128), 128), :] = jnp.zeros((128, dim), jnp.float32)
        return carry

    lax.fori_loop(0, TABLE_BLOCK // 128, clear, 0)
    first, last, flip = start_ref[block], start_ref[block + 1], flip_ref[0]

    def add(k, carry):
        previous, total = carry
        key = key_ref[k]
        row = (key // tokens) & (TABLE_BLOCK - 1)
        value = rows_f32[pl.ds((key & (tokens - 1)) ^ flip, 1), :]
        return row, jnp.where(row == previous, total + value, value)

    def group(g, carry):
        sums = []
        for u in range(UNROLL):
            carry = add(first + g * UNROLL + u, carry)
            sums.append(carry)
        for row, total in sums:
            sums_f32[slot, pl.ds(row, 1), :] = total
        return carry

    def single(k, carry):
        carry = add(k, carry)
        sums_f32[slot, pl.ds(carry[0], 1), :] = carry[1]
        return carry

    carry = (jnp.int32(-1), jnp.zeros((1, dim), jnp.float32))
    groups = (last - first) // UNROLL
    carry = lax.fori_loop(0, groups, group, carry)
    lax.fori_loop(first + groups * UNROLL, last, single, carry)

    @pl.when(block < whole)
    def _():
        put(block, TABLE_BLOCK).start()

    @pl.when(block == blocks - 1)
    def _():
        if rest:
            put(block, rest).start()
        if table_ref.shape[0] > TABLE_BLOCK:
            put(block - 1, TABLE_BLOCK).wait()
        put(block, rest or TABLE_BLOCK).wait()


def table_plan(ids, rank, shard_rows):
    tokens = ids.shape[0]
    local = ids - rank * shard_rows
    owned = (local >= 0) & (local < shard_rows)
    blocks = pl.cdiv(shard_rows, TABLE_BLOCK)
    key = jnp.where(owned, local, shard_rows + TABLE_BLOCK) * tokens + jnp.arange(tokens, dtype=jnp.int32)
    key = lax.sort(key)
    bounds = jnp.minimum(jnp.arange(blocks + 1, dtype=jnp.int32) * TABLE_BLOCK, shard_rows) * tokens
    return jnp.sum((key[None, :] < bounds[:, None]).astype(jnp.int32), axis=1), key


def table_grad(start, key, flip, dx_parts, shard_rows):
    part, dim = dx_parts[0].shape
    return pl.pallas_call(
        table_kernel,
        out_shape=jax.ShapeDtypeStruct((shard_rows, dim), jnp.float32),
        grid_spec=pltpu.PrefetchScalarGridSpec(
            num_scalar_prefetch=3,
            grid=(start.shape[0] - 1,),
            in_specs=[pl.BlockSpec(memory_space=pl.ANY)] * len(dx_parts),
            out_specs=pl.BlockSpec(memory_space=pl.ANY),
            scratch_shapes=[
                pltpu.VMEM((len(dx_parts) * part + 8, dim), jnp.float32),
                pltpu.VMEM((LOAD_DEPTH, part, dim), jnp.bfloat16),
                pltpu.VMEM((2, TABLE_BLOCK + 8, dim), jnp.float32),
                pltpu.SemaphoreType.DMA((LOAD_DEPTH,)),
                pltpu.SemaphoreType.DMA((2,)),
            ],
        ),
        compiler_params=pltpu.CompilerParams(vmem_limit_bytes=58 << 20),
        cost_estimate=pl.CostEstimate(flops=60_000_000_000, bytes_accessed=shard_rows * dim * 4, transcendentals=0),
        name="table_grad",
    )(start, key, flip, *dx_parts)


CORE_SWAP = [(0, 1), (1, 0), (2, 3), (3, 2)]
CHIP_SWAP = [(0, 2), (2, 0), (1, 3), (3, 1)]
DATA_SWAP = [(0, 1), (1, 0)]
ROWS_BY_COLS = (((1,), (0,)), ((), ()))
ROWS_BY_ROWS = (((1,), (1,)), ((), ()))
COLS_BY_COLS = (((0,), (0,)), ((), ()))


def dot(a, b, dims):
    return lax.dot_general(a, b, dims, preferred_element_type=jnp.float32)


def after(value, *others):
    return lax.optimization_barrier((value,) + others)[0]


def solution(mesh):
    tok_spec = P(("pod", "data", "tensor"), None)

    def per_device(token_ids, embed_table, norm_gain, w_in, w_out, d_out):
        shard_rows, dim = embed_table.shape
        tok_dev = d_out.shape[0]
        part = tok_dev // 2
        rank, replica = lax.axis_index("tensor"), lax.axis_index("data")
        chip, core = rank // 2, rank % 2
        gain_f32 = norm_gain.astype(jnp.float32)[None]
        places = token_ids.reshape(2, 2, 2, part)
        places = jnp.where(chip == 0, places[::-1], places)
        places = jnp.where(core == 0, places[:, ::-1], places)
        look = lookup_plan(places.transpose(2, 1, 0, 3).reshape(-1), rank, shard_rows)

        def gather(value):
            from_chip = lax.ppermute(value, "tensor", CHIP_SWAP)
            from_core = lax.ppermute(value, "tensor", CORE_SWAP)
            from_both = lax.ppermute(from_chip, "tensor", CORE_SWAP)
            return value, from_core, from_chip, from_both

        ids_other = lax.ppermute(token_ids, "data", DATA_SWAP)
        ids_low, ids_high = jnp.where(replica == 0, token_ids, ids_other), jnp.where(replica == 0, ids_other, token_ids)
        ids_all = jnp.stack([ids_low, ids_high]).reshape(2, 4, 2, part).transpose(2, 1, 0, 3).reshape(-1)
        start, key = table_plan(ids_all, rank, shard_rows)
        flip = ((rank * 2 + replica) * part).astype(jnp.int32)[None]

        grad_all = []
        for c in range(2):
            pieces = gather(d_out[c * part : (c + 1) * part])
            grad_all.append(join(pieces))

        looked, aways = [], []
        for c in range(2):
            sent = lookup(look, embed_table, 4 * c * part, 2 * part)
            got = lax.ppermute(sent, "tensor", CORE_SWAP)
            kept = lookup(look, embed_table, (4 * c + 2) * part, 2 * part)
            looked.append((kept, got))
            aways.append(lax.ppermute(kept[:part] + got[:part], "tensor", CHIP_SWAP))

        embedded, normed_all = [], []
        for c in range(2):
            x, normed = norm(*looked[c], aways[c], gain_f32)
            embedded.append(x)
            pieces = gather(normed)
            normed_all.append(join(pieces))

        def core_sum(value):
            value = value.reshape(2, 2, part, dim)
            return value, lax.ppermute(value[:, 1], "tensor", CORE_SWAP)

        def chip_sum(value, got, wait_for=None):
            away = value[1, 0] + got[1]
            away = away if wait_for is None else after(away, wait_for)
            return value, got, lax.ppermute(away, "tensor", CHIP_SWAP)

        def up(c):
            return normed_all[c], dot(normed_all[c], w_in, ROWS_BY_COLS).astype(jnp.bfloat16)

        def down(c, pre_gelu):
            gelu_pull = jax.vjp(gelu_tanh, pre_gelu.astype(jnp.float32))[1]
            grad_hidden = dot(grad_all[c], w_out, ROWS_BY_ROWS)
            grad_pre = gelu_pull(grad_hidden)[0].astype(jnp.bfloat16)
            norm_part = dot(grad_pre, w_in, ROWS_BY_ROWS)
            return grad_pre, norm_part, core_sum(norm_part)

        def act(pre_gelu):
            return gelu_tanh(pre_gelu.astype(jnp.float32)).astype(jnp.bfloat16)

        normed_0, pre_0 = up(0)
        grad_pre_0, _, d_normed_0 = down(0, pre_0)
        normed_1, pre_1 = up(1)
        hidden = [act(pre_0), act(pre_1)]
        grad_w_out = dot(hidden[0], grad_all[0], COLS_BY_COLS) + dot(hidden[1], grad_all[1], COLS_BY_COLS)
        cut = grad_w_out.shape[0] // 2
        other_out_0 = lax.ppermute(grad_w_out[:cut], "data", DATA_SWAP)
        grad_pre_1, _, d_normed_1 = down(1, after(pre_1, grad_w_out))

        def to_dx(c, sums):
            return norm_grad(*sums, embedded[c], d_out, c, gain_f32)

        dx_0 = to_dx(0, chip_sum(*d_normed_0))
        crossed_0 = lax.ppermute(dx_0, "data", DATA_SWAP)
        other_out_1 = lax.ppermute(after(grad_w_out[cut:], dx_0), "data", DATA_SWAP)

        grad_pre = [after(g, dx_0) for g in (grad_pre_0, grad_pre_1)]
        grad_w_in = dot(normed_0, grad_pre[0], COLS_BY_COLS) + dot(normed_1, grad_pre[1], COLS_BY_COLS)

        y_sums = []
        for c in range(2):
            mlp_part = dot(hidden[c], w_out, ROWS_BY_COLS)
            y_sums.append(core_sum(mlp_part))

        dx_1 = to_dx(1, chip_sum(*d_normed_1))
        crossed_1 = lax.ppermute(dx_1, "data", DATA_SWAP)
        other_in = lax.ppermute(after(grad_w_in, dx_1), "data", DATA_SWAP)

        dx_all = []
        for dx, crossed in ((dx_0, crossed_0), (dx_1, crossed_1)):
            pair = jnp.concatenate([dx, crossed])
            from_core = lax.ppermute(pair, "tensor", CORE_SWAP)
            from_chip = lax.ppermute(pair, "tensor", CHIP_SWAP)
            from_both = lax.ppermute(from_chip, "tensor", CORE_SWAP)
            dx_all += [pair, from_core, from_chip, from_both]
        y_1 = chip_sum(*y_sums[1], wait_for=from_chip)
        y_0 = chip_sum(*y_sums[0], wait_for=from_chip)
        y_sums = [y_0, y_1]
        grad_table = table_grad(start, key, flip, dx_all, shard_rows)

        block_out = []
        for c, (value, got, away) in enumerate(y_sums):
            mlp_out = (value[0, 0] + got[0]) + after(away, grad_table)
            block_out.append((embedded[c].astype(jnp.float32) + mlp_out).astype(jnp.bfloat16))
        block_out = jnp.concatenate(block_out)
        grad_w_in = grad_w_in + after(other_in, grad_table)
        grad_w_out = grad_w_out + jnp.concatenate([other_out_0, after(other_out_1, grad_table)])
        return block_out, grad_table, grad_w_in, grad_w_out

    return jax.shard_map(
        per_device,
        mesh=mesh,
        in_specs=(P(("pod", "data")), P("tensor", None), P(None), P(None, "tensor"), P("tensor", None), tok_spec),
        out_specs=(tok_spec, P(("pod", "tensor"), None), P("pod", "tensor"), P(("pod", "tensor"), None)),
        check_vma=False,
    )
```

```python
import functools

import jax
import jax.numpy as jnp
from jax import lax
from jax.experimental import pallas as pl
from jax.experimental.pallas import tpu as pltpu
from jax.sharding import PartitionSpec as P


NORM_EPS = 1e-6
LOOK_BLOCK = 256
LOOK_GROUP = 32
LOOK_DEPTH = 3
ISSUE = 16
TABLE_BLOCK = 2048
WIDEN_ROWS = 256
LOAD_DEPTH = 3
UNROLL = 8


def gelu_tanh(value):
    return jax.nn.gelu(value, approximate=True)


def lookup_kernel(base, row_ref, count_ref, code_ref, table_ref, out_ref, tiles, sems):
    step, steps = pl.program_id(0), pl.num_programs(0)

    def fetch(block):
        slot = lax.rem(block, LOOK_DEPTH)
        first = (base + block) * LOOK_BLOCK

        def some(j, carry):
            for k in range(ISSUE):
                row = row_ref[first + j * ISSUE + k]

                @pl.when(row >= 0)
                def _():
                    pltpu.make_async_copy(
                        table_ref.at[pl.ds(pl.multiple_of(row, 8), 8), :],
                        tiles.at[slot * LOOK_BLOCK + j * ISSUE + k],
                        sems.at[slot],
                    ).start()

            return carry

        lax.fori_loop(0, LOOK_BLOCK // ISSUE, some, 0)

    @pl.when(step == 0)
    def _():
        def clear(i, carry):
            tiles[pl.ds(i * LOOK_GROUP, LOOK_GROUP)] = jnp.zeros((LOOK_GROUP,) + tiles.shape[1:], tiles.dtype)
            return carry

        lax.fori_loop(0, LOOK_DEPTH * LOOK_BLOCK // LOOK_GROUP, clear, 0)

        def first(slot, carry):
            fetch(slot)
            return carry

        lax.fori_loop(0, jnp.minimum(LOOK_DEPTH - 1, steps), first, 0)

    @pl.when(step + LOOK_DEPTH - 1 < steps)
    def _():
        fetch(step + LOOK_DEPTH - 1)

    slot = lax.rem(step, LOOK_DEPTH)
    count = count_ref[base + step]

    @pl.when(count > 0)
    def _():
        fetched = tiles.at[pl.ds(0, count)]
        pltpu.make_async_copy(fetched, fetched, sems.at[slot]).wait()

    places = lax.broadcasted_iota(jnp.int32, (LOOK_GROUP * 8, LOOK_GROUP), 0)

    for j in range(LOOK_BLOCK // LOOK_GROUP):
        group = pl.ds(j * LOOK_GROUP, LOOK_GROUP)
        pick = (places == code_ref[pl.ds(j, 1), :]).astype(jnp.bfloat16)
        rows = tiles[pl.ds(slot * LOOK_BLOCK + j * LOOK_GROUP, LOOK_GROUP)].reshape(LOOK_GROUP * 8, -1)
        out_ref[group, :] = dot(pick, rows, COLS_BY_COLS).astype(out_ref.dtype)


def lookup_plan(ids, rank, shard_rows):
    local = ids - rank * shard_rows
    owned = (local >= 0) & (local < shard_rows)
    place = lax.broadcasted_iota(jnp.int32, (ids.shape[0] // LOOK_GROUP, LOOK_GROUP), 1) * 8
    code = jnp.where(owned, local & 7, -1 << 20).reshape(place.shape) + place
    row = jnp.where(owned, local & ~7, -1)
    counts = jnp.sum(owned.reshape(-1, LOOK_BLOCK), axis=1).astype(jnp.int32)
    return row, counts, code


def lookup(plan, table, base, count):
    dim = table.shape[1]
    base //= LOOK_BLOCK
    return pl.pallas_call(
        functools.partial(lookup_kernel, base),
        out_shape=jax.ShapeDtypeStruct((count, dim), table.dtype),
        grid_spec=pltpu.PrefetchScalarGridSpec(
            num_scalar_prefetch=2,
            grid=(count // LOOK_BLOCK,),
            in_specs=[
                pl.BlockSpec((LOOK_BLOCK // LOOK_GROUP, LOOK_GROUP), lambda i, r, c: (base + i, 0)),
                pl.BlockSpec(memory_space=pl.ANY),
            ],
            out_specs=pl.BlockSpec((LOOK_BLOCK, dim), lambda i, r, c: (i, 0)),
            scratch_shapes=[
                pltpu.VMEM((LOOK_DEPTH * LOOK_BLOCK, 8, dim), table.dtype),
                pltpu.SemaphoreType.DMA((LOOK_DEPTH,)),
            ],
        ),
        cost_estimate=pl.CostEstimate(flops=count * 5_000_000, bytes_accessed=count * dim * 18, transcendentals=0),
        name="lookup",
    )(*plan, table)


def norm_kernel(kept_ref, got_ref, away_ref, gain_ref, x_ref, normed_ref):
    x = kept_ref[...].astype(jnp.float32) + got_ref[...].astype(jnp.float32) + away_ref[...].astype(jnp.float32)
    x_ref[...] = x.astype(x_ref.dtype)
    inv_rms = lax.rsqrt(jnp.mean(x * x, axis=-1, keepdims=True) + NORM_EPS)
    normed_ref[...] = (x * inv_rms * gain_ref[...]).astype(normed_ref.dtype)


def norm(kept, got, away, gain):
    rows, dim = away.shape
    tile = rows // 2
    here = pl.BlockSpec((tile, dim), lambda i: (i, 0))
    home = pl.BlockSpec((tile, dim), lambda i: (2 + i, 0))
    return pl.pallas_call(
        norm_kernel,
        out_shape=[jax.ShapeDtypeStruct((rows, dim), away.dtype)] * 2,
        grid=(2,),
        in_specs=[home, home, here, pl.BlockSpec((1, dim), lambda i: (0, 0))],
        out_specs=[here, here],
        cost_estimate=pl.CostEstimate(flops=2_000_000_000, bytes_accessed=rows * dim * 10, transcendentals=rows),
        name="norm",
    )(kept, got, away, gain)


def take_piece(piece_refs, held, sems):
    step = pl.program_id(0)

    @pl.when(step == 0)
    def _():
        for i, piece_ref in enumerate(piece_refs):
            pltpu.make_async_copy(piece_ref, held.at[i], sems.at[i]).start()

    pltpu.make_async_copy(piece_refs[0], held.at[step], sems.at[step]).wait()
    return held[step]


def join_kernel(*refs):
    *piece_refs, out_ref, held, sems = refs
    out_ref[...] = take_piece(piece_refs, held, sems)


def join(pieces):
    (rows, dim), count, kind = pieces[0].shape, len(pieces), pieces[0].dtype
    return pl.pallas_call(
        join_kernel,
        out_shape=jax.ShapeDtypeStruct((count * rows, dim), kind),
        grid=(count,),
        in_specs=[pl.BlockSpec(memory_space=pl.ANY)] * count,
        out_specs=pl.BlockSpec((rows, dim), lambda i: (i, 0)),
        scratch_shapes=[pltpu.VMEM((count, rows, dim), kind), pltpu.SemaphoreType.DMA((count,))],
        cost_estimate=pl.CostEstimate(flops=2_000_000_000, bytes_accessed=count * rows * dim * 4, transcendentals=0),
        name="join",
    )(*pieces)


def dx_kernel(part_ref, got_ref, away_ref, x_ref, grad_ref, gain_ref, dx_ref):
    d_normed = (part_ref[...] + got_ref[...]) + away_ref[...]
    x = x_ref[...].astype(jnp.float32)
    inv_rms = lax.rsqrt(jnp.mean(x * x, axis=-1, keepdims=True) + NORM_EPS)
    x_hat = x * inv_rms
    d_hat = d_normed * gain_ref[...]
    d_norm_in = inv_rms * (d_hat - x_hat * jnp.mean(d_hat * x_hat, axis=-1, keepdims=True))
    dx_ref[...] = (grad_ref[...].astype(jnp.float32) + d_norm_in).astype(dx_ref.dtype)


def norm_grad(part, got, away, x, grad, chunk, gain):
    rows, dim = away.shape
    tile = rows // 2
    plain = pl.BlockSpec((tile, dim), lambda i: (i, 0))
    return pl.pallas_call(
        dx_kernel,
        out_shape=jax.ShapeDtypeStruct((rows, dim), x.dtype),
        grid=(2,),
        in_specs=[
            pl.BlockSpec((None, None, tile, dim), lambda i: (0, 0, i, 0)),
            pl.BlockSpec((None, tile, dim), lambda i: (0, i, 0)),
            plain,
            plain,
            pl.BlockSpec((tile, dim), lambda i: (2 * chunk + i, 0)),
            pl.BlockSpec((1, dim), lambda i: (0, 0)),
        ],
        out_specs=plain,
        cost_estimate=pl.CostEstimate(flops=3_000_000_000, bytes_accessed=rows * dim * 18, transcendentals=rows),
        name="norm_grad",
    )(part, got, away, x, grad, gain)


def table_kernel(start_ref, key_ref, flip_ref, *refs):
    *dx_refs, table_ref, rows_f32, stage, sums_f32, sems, out_sems = refs
    block, blocks = pl.program_id(0), pl.num_programs(0)
    part, dim = dx_refs[0].shape
    tokens = len(dx_refs) * part

    @pl.when(block == 0)
    def _():
        def load(i):
            return pltpu.make_async_copy(dx_refs[i], stage.at[i % LOAD_DEPTH], sems.at[i % LOAD_DEPTH])

        for i in range(LOAD_DEPTH - 1):
            load(i).start()
        for i in range(len(dx_refs)):
            if i + LOAD_DEPTH - 1 < len(dx_refs):
                load(i + LOAD_DEPTH - 1).start()
            load(i).wait()

            def widen(j, carry, i=i):
                rows = pl.ds(pl.multiple_of(j * WIDEN_ROWS, WIDEN_ROWS), WIDEN_ROWS)
                wide = pl.ds(pl.multiple_of(i * part + j * WIDEN_ROWS, WIDEN_ROWS), WIDEN_ROWS)
                rows_f32[wide, :] = stage[i % LOAD_DEPTH, rows, :].astype(jnp.float32)
                return carry

            lax.fori_loop(0, part // WIDEN_ROWS, widen, 0)

    slot = lax.rem(block, 2)
    whole, rest = table_ref.shape[0] // TABLE_BLOCK, table_ref.shape[0] % TABLE_BLOCK

    def put(i, rows):
        at = lax.rem(i, 2)
        return pltpu.make_async_copy(
            sums_f32.at[at, pl.ds(0, rows), :],
            table_ref.at[pl.ds(pl.multiple_of(i * TABLE_BLOCK, TABLE_BLOCK), rows), :],
            out_sems.at[at],
        )

    @pl.when(block >= 2)
    def _():
        put(block - 2, TABLE_BLOCK).wait()

    def clear(i, carry):
        sums_f32[slot, pl.ds(pl.multiple_of(i * 128, 128), 128), :] = jnp.zeros((128, dim), jnp.float32)
        return carry

    lax.fori_loop(0, TABLE_BLOCK // 128, clear, 0)
    first, last, flip = start_ref[block], start_ref[block + 1], flip_ref[0]

    def add(k, carry):
        previous, total = carry
        key = key_ref[k]
        row = (key // tokens) & (TABLE_BLOCK - 1)
        value = rows_f32[pl.ds((key & (tokens - 1)) ^ flip, 1), :]
        return row, jnp.where(row == previous, total + value, value)

    def group(g, carry):
        sums = []
        for u in range(UNROLL):
            carry = add(first + g * UNROLL + u, carry)
            sums.append(carry)
        for row, total in sums:
            sums_f32[slot, pl.ds(row, 1), :] = total
        return carry

    def single(k, carry):
        carry = add(k, carry)
        sums_f32[slot, pl.ds(carry[0], 1), :] = carry[1]
        return carry

    carry = (jnp.int32(-1), jnp.zeros((1, dim), jnp.float32))
    groups = (last - first) // UNROLL
    carry = lax.fori_loop(0, groups, group, carry)
    lax.fori_loop(first + groups * UNROLL, last, single, carry)

    @pl.when(block < whole)
    def _():
        put(block, TABLE_BLOCK).start()

    @pl.when(block == blocks - 1)
    def _():
        if rest:
            put(block, rest).start()
        if table_ref.shape[0] > TABLE_BLOCK:
            put(block - 1, TABLE_BLOCK).wait()
        put(block, rest or TABLE_BLOCK).wait()


def table_plan(ids, rank, shard_rows):
    tokens = ids.shape[0]
    local = ids - rank * shard_rows
    owned = (local >= 0) & (local < shard_rows)
    blocks = pl.cdiv(shard_rows, TABLE_BLOCK)
    key = jnp.where(owned, local, shard_rows + TABLE_BLOCK) * tokens + jnp.arange(tokens, dtype=jnp.int32)
    key = lax.sort(key)
    bounds = jnp.minimum(jnp.arange(blocks + 1, dtype=jnp.int32) * TABLE_BLOCK, shard_rows) * tokens
    return jnp.sum((key[None, :] < bounds[:, None]).astype(jnp.int32), axis=1), key


def table_grad(start, key, flip, dx_parts, shard_rows):
    part, dim = dx_parts[0].shape
    return pl.pallas_call(
        table_kernel,
        out_shape=jax.ShapeDtypeStruct((shard_rows, dim), jnp.float32),
        grid_spec=pltpu.PrefetchScalarGridSpec(
            num_scalar_prefetch=3,
            grid=(start.shape[0] - 1,),
            in_specs=[pl.BlockSpec(memory_space=pl.ANY)] * len(dx_parts),
            out_specs=pl.BlockSpec(memory_space=pl.ANY),
            scratch_shapes=[
                pltpu.VMEM((len(dx_parts) * part + 8, dim), jnp.float32),
                pltpu.VMEM((LOAD_DEPTH, part, dim), jnp.bfloat16),
                pltpu.VMEM((2, TABLE_BLOCK + 8, dim), jnp.float32),
                pltpu.SemaphoreType.DMA((LOAD_DEPTH,)),
                pltpu.SemaphoreType.DMA((2,)),
            ],
        ),
        compiler_params=pltpu.CompilerParams(vmem_limit_bytes=58 << 20),
        cost_estimate=pl.CostEstimate(flops=60_000_000_000, bytes_accessed=shard_rows * dim * 4, transcendentals=0),
        name="table_grad",
    )(start, key, flip, *dx_parts)


CORE_SWAP = [(0, 1), (1, 0), (2, 3), (3, 2)]
CHIP_SWAP = [(0, 2), (2, 0), (1, 3), (3, 1)]
DATA_SWAP = [(0, 1), (1, 0)]
ROWS_BY_COLS = (((1,), (0,)), ((), ()))
ROWS_BY_ROWS = (((1,), (1,)), ((), ()))
COLS_BY_COLS = (((0,), (0,)), ((), ()))


def dot(a, b, dims):
    return lax.dot_general(a, b, dims, preferred_element_type=jnp.float32)


def after(value, *others):
    return lax.optimization_barrier((value,) + others)[0]


def solution(mesh):
    tok_spec = P(("pod", "data", "tensor"), None)

    def per_device(token_ids, embed_table, norm_gain, w_in, w_out, d_out):
        shard_rows, dim = embed_table.shape
        tok_dev = d_out.shape[0]
        part = tok_dev // 2
        rank, replica = lax.axis_index("tensor"), lax.axis_index("data")
        chip, core = rank // 2, rank % 2
        gain_f32 = norm_gain.astype(jnp.float32)[None]
        places = token_ids.reshape(2, 2, 2, part)
        places = jnp.where(chip == 0, places[::-1], places)
        places = jnp.where(core == 0, places[:, ::-1], places)
        look = lookup_plan(places.transpose(2, 1, 0, 3).reshape(-1), rank, shard_rows)

        def gather(value):
            from_chip = lax.ppermute(value, "tensor", CHIP_SWAP)
            from_core = lax.ppermute(value, "tensor", CORE_SWAP)
            from_both = lax.ppermute(from_chip, "tensor", CORE_SWAP)
            return value, from_core, from_chip, from_both

        ids_other = lax.ppermute(token_ids, "data", DATA_SWAP)
        ids_low, ids_high = jnp.where(replica == 0, token_ids, ids_other), jnp.where(replica == 0, ids_other, token_ids)
        ids_all = jnp.stack([ids_low, ids_high]).reshape(2, 4, 2, part).transpose(2, 1, 0, 3).reshape(-1)
        start, key = table_plan(ids_all, rank, shard_rows)
        flip = ((rank * 2 + replica) * part).astype(jnp.int32)[None]

        grad_all = []
        for c in range(2):
            pieces = gather(d_out[c * part : (c + 1) * part])
            grad_all.append(join(pieces))

        looked, aways = [], []
        for c in range(2):
            sent = lookup(look, embed_table, 4 * c * part, 2 * part)
            got = lax.ppermute(sent, "tensor", CORE_SWAP)
            kept = lookup(look, embed_table, (4 * c + 2) * part, 2 * part)
            looked.append((kept, got))
            aways.append(lax.ppermute(kept[:part] + got[:part], "tensor", CHIP_SWAP))

        embedded, normed_all = [], []
        for c in range(2):
            x, normed = norm(*looked[c], aways[c], gain_f32)
            embedded.append(x)
            pieces = gather(normed)
            normed_all.append(join(pieces))

        def core_sum(value):
            value = value.reshape(2, 2, part, dim)
            return value, lax.ppermute(value[:, 1], "tensor", CORE_SWAP)

        def chip_sum(value, got, wait_for=None):
            away = value[1, 0] + got[1]
            away = away if wait_for is None else after(away, wait_for)
            return value, got, lax.ppermute(away, "tensor", CHIP_SWAP)

        def up(c):
            return normed_all[c], dot(normed_all[c], w_in, ROWS_BY_COLS).astype(jnp.bfloat16)

        def down(c, pre_gelu):
            gelu_pull = jax.vjp(gelu_tanh, pre_gelu.astype(jnp.float32))[1]
            grad_hidden = dot(grad_all[c], w_out, ROWS_BY_ROWS)
            grad_pre = gelu_pull(grad_hidden)[0].astype(jnp.bfloat16)
            norm_part = dot(grad_pre, w_in, ROWS_BY_ROWS)
            return grad_pre, norm_part, core_sum(norm_part)

        def act(pre_gelu):
            return gelu_tanh(pre_gelu.astype(jnp.float32)).astype(jnp.bfloat16)

        normed_0, pre_0 = up(0)
        grad_pre_0, _, d_normed_0 = down(0, pre_0)
        normed_1, pre_1 = up(1)
        hidden = [act(pre_0), act(pre_1)]
        grad_w_out = dot(hidden[0], grad_all[0], COLS_BY_COLS) + dot(hidden[1], grad_all[1], COLS_BY_COLS)
        cut = grad_w_out.shape[0] // 2
        other_out_0 = lax.ppermute(grad_w_out[:cut], "data", DATA_SWAP)
        grad_pre_1, _, d_normed_1 = down(1, after(pre_1, grad_w_out))

        def to_dx(c, sums):
            return norm_grad(*sums, embedded[c], d_out, c, gain_f32)

        dx_0 = to_dx(0, chip_sum(*d_normed_0))
        crossed_0 = lax.ppermute(dx_0, "data", DATA_SWAP)
        other_out_1 = lax.ppermute(grad_w_out[cut : cut + 128], "data", DATA_SWAP)
        other_out_2 = lax.ppermute(after(grad_w_out[cut + 128 :], dx_0), "data", DATA_SWAP)

        grad_pre = [after(g, dx_0) for g in (grad_pre_0, grad_pre_1)]
        grad_w_in = dot(normed_0, grad_pre[0], COLS_BY_COLS) + dot(normed_1, grad_pre[1], COLS_BY_COLS)

        y_sums = []
        for c in range(2):
            mlp_part = dot(hidden[c], w_out, ROWS_BY_COLS)
            y_sums.append(core_sum(mlp_part))

        dx_1 = to_dx(1, chip_sum(*d_normed_1))
        crossed_1 = lax.ppermute(dx_1, "data", DATA_SWAP)
        other_in = lax.ppermute(after(grad_w_in, dx_1), "data", DATA_SWAP)

        dx_all = []
        for dx, crossed in ((dx_0, crossed_0), (dx_1, crossed_1)):
            pair = jnp.concatenate([dx, crossed])
            from_core = lax.ppermute(pair, "tensor", CORE_SWAP)
            from_chip = lax.ppermute(pair, "tensor", CHIP_SWAP)
            from_both = lax.ppermute(from_chip, "tensor", CORE_SWAP)
            dx_all += [pair, from_core, from_chip, from_both]
        y_1 = chip_sum(*y_sums[1], wait_for=from_chip)
        y_0 = chip_sum(*y_sums[0], wait_for=from_chip)
        y_sums = [y_0, y_1]
        grad_table = table_grad(start, key, flip, dx_all, shard_rows)

        block_out = []
        for c, (value, got, away) in enumerate(y_sums):
            mlp_out = (value[0, 0] + got[0]) + after(away, grad_table)
            block_out.append((embedded[c].astype(jnp.float32) + mlp_out).astype(jnp.bfloat16))
        block_out = jnp.concatenate(block_out)
        grad_w_in = grad_w_in + after(other_in, grad_table)
        grad_w_out = grad_w_out + jnp.concatenate([other_out_0, other_out_1, after(other_out_2, grad_table)])
        return block_out, grad_table, grad_w_in, grad_w_out

    return jax.shard_map(
        per_device,
        mesh=mesh,
        in_specs=(P(("pod", "data")), P("tensor", None), P(None), P(None, "tensor"), P("tensor", None), tok_spec),
        out_specs=(tok_spec, P(("pod", "tensor"), None), P("pod", "tensor"), P(("pod", "tensor"), None)),
        check_vma=False,
    )
```
